32 devices in a mesh: group: 2 (over y), seq: 16 (over z, x, core), tensor: 1.
Axes of the slice: x: 2, y: 2, z: 4, core: 2. Of those that a mesh axis runs over, the one named last changes fastest.
Arguments:
- queries: bfloat16 [64, 64, 128], P('group', 'tensor'), parts along dimension 0, may hold values from -10 to 10
- k_cache: bfloat16 [256, 8, 128, 128], P(('group', 'seq'), 'tensor'), parts along dimension 0, may hold values from -6 to 6
- value_cache: bfloat16 [256, 8, 128, 128], P(('group', 'seq'), 'tensor'), parts along dimension 0, may hold values from -6 to 6
- kv_lengths: int32 [64], P('group'), parts along dimension 0, may hold values from 1 to 4096, as said below
- page_table: int32 [64, 32], P('group'), parts along dimension 0, may hold values from -1 to 127, as said below
- request_batch_row: int32 [64], P('group'), parts along dimension 0, may hold values from 0 to 31, each once
Outputs:
- attended: bfloat16 [64, 64, 128], P('group', 'tensor'), parts along dimension 0
The draws below stay inside these ranges and needn't reach their ends.
There are 2 independent parts, one for each index of `group`. The reference program is written for one: setup_inputs(seed, part) draws one part's arguments, and reference() takes and returns one part's arrays. A program takes and returns all parts, laid end to end along the dimension named above; each array names one. Nothing has to cross between parts.
Inputs may be any that keep to these rules, and one draw needn't show every extreme that they name: `kv_lengths`: the longest request holds exactly 4096 tokens. `page_table`: row r lists in order the cache slots of the first ceil(kv_lengths[r] / 128) pages of request r and -1 after them; no slot is listed twice.
All inputs are finite; a program needn't handle non-finite values.
Results may differ from the reference program's by a relative error of at most 0.0042.
Values may be sent and summed in bfloat16 or wider, within the bound.
A program may use at most 64 MiB of HBM per device.

```python
import jax
import jax.numpy as jnp
from jax import lax

QUERY_HEADS = 64
KEY_VALUE_HEADS = 8
HEAD_WIDTH = 128
PAGE_TOKENS = 128
REQS = 32
POOL_SLOTS = 128
MAXPAGES = 32


def page_plan(key):
    plan_key = jax.random.fold_in(key, 31)
    key_counts, key_long, key_tail, key_slots = jax.random.split(plan_key, 4)
    request_ids = jnp.arange(REQS, dtype=jnp.int32)
    ceiling = POOL_SLOTS // 4 // (REQS - 1)
    counts = jax.random.randint(key_counts, (REQS,), 1, ceiling + 1, dtype=jnp.int32)
    longest = jax.random.randint(key_long, (), 0, REQS, dtype=jnp.int32)
    counts = jnp.where(request_ids == longest, MAXPAGES, counts).astype(jnp.int32)
    tail_tokens = jax.random.randint(key_tail, (REQS,), 1, PAGE_TOKENS + 1, dtype=jnp.int32)
    lengths = jnp.where(request_ids == longest, MAXPAGES * PAGE_TOKENS, (counts - 1) * PAGE_TOKENS + tail_tokens)
    shuffled = jax.random.permutation(key_slots, POOL_SLOTS).astype(jnp.int32)
    starts = jnp.cumsum(counts) - counts
    page_ids = jnp.arange(MAXPAGES, dtype=jnp.int32)
    slot_index = jnp.clip(starts[:, None] + page_ids[None, :], 0, POOL_SLOTS - 1)
    page_rows = jnp.where(page_ids[None, :] < counts[:, None], jnp.take(shuffled, slot_index), -1)
    return (lengths.astype(jnp.int32), page_rows.astype(jnp.int32))


def draw_kv_lengths(key, part):
    return page_plan(key)[0]


def draw_page_table(key, part):
    return page_plan(key)[1]


def draw_queries(key, part):
    values = jnp.clip(jax.random.normal(jax.random.fold_in(key, 11), (REQS, QUERY_HEADS, HEAD_WIDTH), jnp.float32), -6.0, 6.0)
    return values.astype(jnp.bfloat16)


def draw_k_cache(key, part):
    cache_layout = (POOL_SLOTS, KEY_VALUE_HEADS, PAGE_TOKENS, HEAD_WIDTH)
    values = jnp.clip(jax.random.normal(jax.random.fold_in(key, 13), cache_layout, jnp.float32), -6.0, 6.0)
    return values.astype(jnp.bfloat16)


def shard_levels(stream_key, extent, cuts, low, top_value):
    def one(axis_at, parts):
        steps = jax.random.uniform(jax.random.fold_in(jax.random.fold_in(stream_key, 6), axis_at), (parts,), jnp.float32, low / len(cuts), top_value / len(cuts))
        return jnp.repeat(jnp.exp(steps), extent[axis_at] // parts).reshape((-1,) + (1,) * (len(extent) - axis_at - 1))

    factor_of = one(*cuts[0])
    for cut in cuts[1:]:
        factor_of = factor_of * one(*cut)
    return factor_of


def normal_values(rng, shape, deviation, limit, shards=(), kind=jnp.bfloat16):
    result = jax.random.normal(rng, shape, jnp.float32) * deviation
    if len(shards) > 0:
        result = shard_levels(rng, shape, shards, -0.22, 0.18) * result
    return jnp.clip(result, min=-limit, max=limit).astype(kind)


def setup_inputs(seed: int = 0, part: int = 0) -> dict:
    keys = jax.random.split(jax.random.key(seed), 7)
    part_keys = jax.random.split(jax.random.fold_in(keys[6], part), 7)
    return {
        "queries": draw_queries(jax.random.fold_in(jax.random.fold_in(keys[6], part), 71), part),
        "k_cache": draw_k_cache(jax.random.fold_in(jax.random.fold_in(keys[6], part), 71), part),
        "value_cache": normal_values(part_keys[2], (POOL_SLOTS, KEY_VALUE_HEADS, PAGE_TOKENS, HEAD_WIDTH), 1.0, 6.0, ((0, 16),)),
        "kv_lengths": draw_kv_lengths(jax.random.fold_in(jax.random.fold_in(keys[6], part), 71), part),
        "page_table": draw_page_table(jax.random.fold_in(jax.random.fold_in(keys[6], part), 71), part),
        "request_batch_row": jax.random.permutation(part_keys[5], REQS).astype(jnp.int32),
    }


NEG_BIG = -1.0e30


def reference(queries, k_cache, value_cache, kv_lengths, page_table, request_batch_row):
    group_width = QUERY_HEADS // KEY_VALUE_HEADS
    scale = HEAD_WIDTH ** -0.5

    def one_request(request_number):
        slot_rows = jnp.maximum(page_table[request_number], 0).astype(jnp.int32)
        key_pages = jnp.take(k_cache, slot_rows, axis=0).astype(jnp.float32)
        value_pages = jnp.take(value_cache, slot_rows, axis=0).astype(jnp.float32)
        query_head_rows = queries[request_batch_row[request_number]].astype(jnp.float32).reshape(KEY_VALUE_HEADS, group_width, HEAD_WIDTH)
        scores = jnp.einsum("kgd,pktd->pkgt", query_head_rows, key_pages) * scale
        positions = jnp.arange(MAXPAGES * PAGE_TOKENS, dtype=jnp.int32).reshape(MAXPAGES, PAGE_TOKENS)
        valid_mask = (positions < kv_lengths[request_number])[:, None, None, :]
        masked = jnp.where(valid_mask, scores, NEG_BIG)
        page_max = jnp.max(masked, axis=3)
        weights = jnp.where(valid_mask, jnp.exp(masked - page_max[..., None]), 0.0)
        page_sum = jnp.sum(weights, axis=3)
        weights_bf = lax.optimization_barrier(weights.astype(jnp.bfloat16))
        page_out = jnp.einsum("pkgt,pktd->pkgd", weights_bf.astype(jnp.float32), value_pages)
        request_top = jnp.max(page_max, axis=0)
        factor = jnp.exp(page_max - request_top[None])
        total_sum = jnp.sum(page_sum * factor, axis=0)
        total_out = jnp.sum(page_out * factor[..., None], axis=0)
        return (total_out / total_sum[..., None]).astype(jnp.bfloat16).reshape(QUERY_HEADS, HEAD_WIDTH)

    results = lax.map(one_request, jnp.arange(REQS, dtype=jnp.int32))
    return jnp.zeros((REQS, QUERY_HEADS, HEAD_WIDTH), jnp.bfloat16).at[request_batch_row].set(results)
```

```python
import functools

import jax
import jax.numpy as jnp
from jax import lax
from jax.experimental import pallas as pl
from jax.experimental.pallas import tpu as pltpu
from jax.sharding import PartitionSpec as P

NEG_BIG = -1e30


def slot_owners(page_table, first_slot, slot_count):
    global_ids = first_slot + jnp.arange(slot_count, dtype=jnp.int32)
    match_int = (page_table[None, :, :] == global_ids[:, None, None]).astype(jnp.int32)
    request_ids = jnp.arange(page_table.shape[0], dtype=jnp.int32)
    page_ids = jnp.arange(page_table.shape[1], dtype=jnp.int32)
    owner_ids = jnp.sum(match_int * request_ids[None, :, None], axis=(1, 2))
    logical = jnp.sum(match_int * page_ids[None, None, :], axis=(1, 2))
    live_mask = jnp.sum(match_int, axis=(1, 2)) > 0
    return (owner_ids, logical, live_mask)


def page_partials(q_rows, key_pages, value_pages, owner_ids, logical, live_mask, kv_lengths):
    slot_count, heads_kv, page_len, head_dim = key_pages.shape
    group_width = q_rows.shape[1] // heads_kv
    slot_queries = jnp.take(q_rows, owner_ids, axis=0).reshape(
        slot_count, heads_kv, group_width, head_dim
    )
    scores = jnp.einsum(
        "skgd,sktd->skgt", slot_queries, key_pages, preferred_element_type=jnp.float32
    ) * head_dim ** (-0.5)
    positions = logical[:, None] * page_len + jnp.arange(page_len, dtype=jnp.int32)[None, :]
    valid_mask = live_mask[:, None] & (positions < jnp.take(kv_lengths, owner_ids)[:, None])
    valid_wide = valid_mask[:, None, None, :]
    masked = jnp.where(valid_wide, scores, NEG_BIG)
    page_max = jnp.max(masked, axis=3)
    weights = jnp.where(valid_wide, jnp.exp(masked - page_max[..., None]), 0.0)
    page_sum = jnp.sum(weights, axis=3)
    page_out = jnp.einsum(
        "skgt,sktd->skgd",
        weights.astype(jnp.bfloat16),
        value_pages,
        preferred_element_type=jnp.float32,
    )
    return (
        page_max.reshape(slot_count, -1),
        page_sum.reshape(slot_count, -1),
        page_out.reshape(slot_count, -1),
    )


def request_partials(page_max, page_sum, page_out, owner_ids, live_mask, requests, head_dim):
    slot_count, heads_local = page_max.shape
    owned = (owner_ids[:, None] == jnp.arange(requests, dtype=jnp.int32)[None, :]) & live_mask[
        :, None
    ]
    req_max = jnp.max(jnp.where(owned[:, :, None], page_max[:, None, :], NEG_BIG), axis=0)
    factor = jnp.where(
        live_mask[:, None], jnp.exp(page_max - jnp.take(req_max, owner_ids, axis=0)), 0.0
    )
    owned_float = owned.astype(jnp.float32)
    req_sum = jnp.einsum(
        "sr,sh->rh", owned_float, page_sum * factor, precision=lax.Precision.HIGHEST
    )
    scaled = (page_out.reshape(slot_count, heads_local, head_dim) * factor[..., None]).reshape(
        slot_count, -1
    )
    req_out = jnp.einsum("sr,sx->rx", owned_float, scaled, precision=lax.Precision.HIGHEST)
    return (req_max, req_sum, req_out.reshape(requests, heads_local, head_dim))


def plain_shards(queries, k_cache, value_cache, kv_lengths, page_table, request_batch_row):
    slot_count = k_cache.shape[0]
    requests = queries.shape[0]
    heads_local = queries.shape[1]
    head_dim = queries.shape[2]
    first_slot = lax.axis_index("seq") * slot_count
    owner_ids, logical, live_mask = slot_owners(page_table, first_slot, slot_count)
    q_rows = jnp.take(queries, request_batch_row, axis=0)
    page_max, page_sum, page_out = page_partials(
        q_rows, k_cache, value_cache, owner_ids, logical, live_mask, kv_lengths
    )
    owner_used, live_used = (owner_ids, live_mask)
    req_max, req_sum, req_out = request_partials(
        page_max, page_sum, page_out, owner_used, live_used, requests, head_dim
    )
    overall = lax.pmax(req_max, "seq")
    factor = jnp.exp(req_max - overall)
    flat_sum = (req_sum * factor).reshape(-1)
    flat_out = (req_out * factor[..., None]).reshape(requests * heads_local, head_dim)
    part_out, part_sum = (
        lax.psum_scatter(flat_out, "seq", scatter_dimension=0, tiled=True),
        lax.psum_scatter(flat_sum, "seq", scatter_dimension=0, tiled=True),
    )
    finished = (part_out / part_sum[:, None]).astype(jnp.bfloat16)
    result = lax.all_gather(finished, "seq", axis=0, tiled=True).reshape(
        requests, heads_local, head_dim
    )
    return jnp.zeros_like(queries).at[request_batch_row].set(result)


def attend_kernel(
    n,
    rows_smem,
    lens_smem,
    rows_ref,
    table_ref,
    q_ref,
    k_hbm,
    v_hbm,
    out_ref,
    k_buf,
    v_buf,
    part,
    x_send,
    x_recv,
    l_send,
    l_recv,
    piece,
    k_sem,
    v_sem,
    xs_sem,
    xr_sem,
    ls_sem,
    lr_sem,
    gs_sem,
    gr_sem,
    fs_sem,
    fr_sem,
    own_sem,
):
    me = lax.axis_index("seq")
    slots, heads_kv, page_len, head_dim = k_hbm.shape
    requests, heads, _ = q_ref.shape
    width = heads // heads_kv
    mine = heads // n
    pages = table_ref.shape[1]
    total_slots = n * slots

    def remote(src, dst, send_sem, recv_sem, target):
        return pltpu.make_async_remote_copy(
            src_ref=src,
            dst_ref=dst,
            send_sem=send_sem,
            recv_sem=recv_sem,
            device_id={"seq": target},
            device_id_type=pl.DeviceIdType.MESH,
        )

    k_copies = [pltpu.make_async_copy(k_hbm.at[s], k_buf.at[s], k_sem.at[s]) for s in range(slots)]
    v_copies = [pltpu.make_async_copy(v_hbm.at[s], v_buf.at[s], v_sem.at[s]) for s in range(slots)]
    for s in range(slots):
        k_copies[s].start()
        v_copies[s].start()

    barrier = pltpu.get_barrier_semaphore()
    for o in range(1, n):
        pl.semaphore_signal(
            barrier,
            inc=1,
            device_id={"seq": lax.rem(me + o, n)},
            device_id_type=pl.DeviceIdType.MESH,
        )

    table = table_ref[...]
    code = lax.broadcasted_iota(jnp.int32, table.shape, 0) * pages + lax.broadcasted_iota(
        jnp.int32, table.shape, 1
    )
    found = []
    for s in range(slots):
        found.append(jnp.max(jnp.where(table == me * slots + s, code, -1)))

    lane = lax.broadcasted_iota(jnp.int32, (1, total_slots), 1)
    token = lax.broadcasted_iota(jnp.int32, (1, page_len), 1)
    lse = jnp.zeros((heads, total_slots), jnp.float32)
    for s in range(slots):
        at = jnp.maximum(found[s], 0)
        request = at // pages
        page = at - request * pages
        left = jnp.where(found[s] >= 0, lens_smem[request] - page * page_len, 0)
        q_rows = q_ref[rows_smem[request]]
        k_copies[s].wait()
        scores = jnp.concatenate(
            [
                lax.dot_general(
                    q_rows[g * width : (g + 1) * width],
                    k_buf[s, g],
                    (((1,), (1,)), ((), ())),
                    preferred_element_type=jnp.float32,
                )
                for g in range(heads_kv)
            ],
            axis=0,
        ) * head_dim ** (-0.5)
        masked = jnp.where(token < left, scores, NEG_BIG)
        top = jnp.max(masked, axis=1, keepdims=True)
        weights = jnp.exp(masked - top)
        weight_sum = jnp.sum(weights, axis=1, keepdims=True)
        lse = jnp.where(lane == me * slots + s, top + jnp.log(weight_sum), lse)
        weights_bf = weights.astype(jnp.bfloat16)
        inverse = 1.0 / weight_sum
        v_copies[s].wait()
        for g in range(heads_kv):
            band = slice(g * width, (g + 1) * width)
            out = jnp.dot(weights_bf[band], v_buf[s, g], preferred_element_type=jnp.float32)
            part[band, s, :] = out * inverse[band]

    l_send[...] = lse.reshape(n, mine, total_slots)
    for j in range(n):
        x_send[j] = part[j * mine : (j + 1) * mine].astype(jnp.bfloat16)

    pl.semaphore_wait(barrier, n - 1)
    first = []
    for o in range(1, n):
        to = lax.rem(me + o, n)
        first.append(remote(l_send.at[to], l_recv.at[me], ls_sem.at[o], lr_sem.at[me], to))
        first.append(remote(x_send.at[to], x_recv.at[me], xs_sem.at[o], xr_sem.at[me], to))
    for copy in first:
        copy.start()

    x_recv[me] = x_send[me]
    l_recv[me] = l_send[me]
    owned = jnp.zeros((requests, total_slots), jnp.bool_)
    for p in range(pages):
        owned = owned | (table[:, p : p + 1] == lane)
    place = (
        lax.broadcasted_iota(jnp.int32, (requests, requests), 0) == rows_ref[...]
    ).astype(jnp.float32).astype(jnp.bfloat16)
    owned = (
        jnp.dot(
            place,
            owned.astype(jnp.float32).astype(jnp.bfloat16),
            preferred_element_type=jnp.float32,
        )
        > 0.5
    )

    for o in range(1, n):
        source = lax.rem(me + o, n)
        remote(l_send.at[0], l_recv.at[source], ls_sem.at[0], lr_sem.at[source], source).wait_recv()
    lse_all = l_recv[0]
    for j in range(1, n):
        lse_all = lse_all + l_recv[j]
    mixes = []
    for h in range(mine):
        level = jnp.where(owned, lse_all[h : h + 1], NEG_BIG)
        peak = jnp.max(level, axis=1, keepdims=True)
        mix = jnp.where(owned, jnp.exp(level - peak), 0.0)
        mix = mix * (1.0 / jnp.sum(mix, axis=1, keepdims=True))
        high = mix.astype(jnp.bfloat16)
        low = (mix - high.astype(jnp.float32)).astype(jnp.bfloat16)
        mixes.append((high, low))
    for o in range(1, n):
        source = lax.rem(me + o, n)
        remote(x_send.at[0], x_recv.at[source], xs_sem.at[0], xr_sem.at[source], source).wait_recv()
    for h in range(mine):
        rows = jnp.concatenate([x_recv[j, h].astype(jnp.float32) for j in range(n)], axis=0).astype(
            jnp.bfloat16
        )
        high, low = mixes[h]
        done = jnp.dot(high, rows, preferred_element_type=jnp.float32) + jnp.dot(
            low, rows, preferred_element_type=jnp.float32
        )
        piece[h] = done.astype(jnp.bfloat16)

    partner = me + 1 - 2 * lax.rem(me, 2)
    second = []
    for o in range(2, n, 2):
        to = lax.rem(me + o, n)
        second.append(remote(piece, out_ref.at[me], gs_sem.at[o], gr_sem.at[me], to))
    second.append(remote(piece, out_ref.at[me], fs_sem.at[0], fr_sem.at[me], partner))
    for copy in second:
        copy.start()
    own = pltpu.make_async_copy(piece, out_ref.at[me], own_sem)
    own.start()
    passed = []
    for o in range(2, n, 2):
        source = lax.rem(me + o, n)
        remote(piece, out_ref.at[source], gs_sem.at[0], gr_sem.at[source], source).wait_recv()
        on = remote(
            out_ref.at[source], out_ref.at[source], fs_sem.at[o], fr_sem.at[source], partner
        )
        on.start()
        passed.append(on)
    for o in range(0, n, 2):
        source = lax.rem(partner + o, n)
        remote(piece, out_ref.at[source], fs_sem.at[0], fr_sem.at[source], partner).wait_recv()
    own.wait()
    for copy in first + second + passed:
        copy.wait_send()


def seq_shards(n, queries, k_cache, value_cache, kv_lengths, page_table, request_batch_row):
    slots, heads_kv, page_len, head_dim = k_cache.shape
    requests, heads, _ = queries.shape
    if heads % n or n % 2:
        return plain_shards(
            queries, k_cache, value_cache, kv_lengths, page_table, request_batch_row
        )
    mine = heads // n
    smem = pl.BlockSpec(memory_space=pltpu.SMEM)
    vmem = pl.BlockSpec(memory_space=pltpu.VMEM)
    anywhere = pl.BlockSpec(memory_space=pl.ANY)
    sems = pltpu.SemaphoreType.DMA
    out = pl.pallas_call(
        functools.partial(attend_kernel, n),
        out_shape=jax.ShapeDtypeStruct((n, mine, requests, head_dim), queries.dtype),
        in_specs=[smem, smem, vmem, vmem, vmem, anywhere, anywhere],
        out_specs=vmem,
        scratch_shapes=[
            pltpu.VMEM(k_cache.shape, k_cache.dtype),
            pltpu.VMEM(value_cache.shape, value_cache.dtype),
            pltpu.VMEM((heads, slots, head_dim), jnp.float32),
            pltpu.VMEM((n, mine, slots, head_dim), jnp.bfloat16),
            pltpu.VMEM((n, mine, slots, head_dim), jnp.bfloat16),
            pltpu.VMEM((n, mine, n * slots), jnp.float32),
            pltpu.VMEM((n, mine, n * slots), jnp.float32),
            pltpu.VMEM((mine, requests, head_dim), jnp.bfloat16),
            sems((slots,)),
            sems((slots,)),
            sems((n,)),
            sems((n,)),
            sems((n,)),
            sems((n,)),
            sems((n,)),
            sems((n,)),
            sems((n,)),
            sems((n,)),
            sems,
        ],
        compiler_params=pltpu.CompilerParams(collective_id=0, has_side_effects=True),
    )(
        request_batch_row,
        kv_lengths,
        request_batch_row.reshape(1, requests),
        page_table,
        queries,
        k_cache,
        value_cache,
    )
    return out.reshape(heads, requests, head_dim).transpose(1, 0, 2)


def solution(mesh):
    shards = functools.partial(seq_shards, mesh.shape["seq"])
    return jax.shard_map(
        shards,
        mesh=mesh,
        in_specs=(
            P("group", "tensor", None),
            P(("group", "seq"), "tensor", None, None),
            P(("group", "seq"), "tensor", None, None),
            P("group"),
            P("group", None),
            P("group"),
        ),
        out_specs=P("group", "tensor", None),
        check_vma=False,
    )
```

```python
import functools

import jax
import jax.numpy as jnp
from jax import lax
from jax.experimental import pallas as pl
from jax.experimental.pallas import tpu as pltpu
from jax.sharding import PartitionSpec as P

NEG_BIG = -1e30


def slot_owners(page_table, first_slot, slot_count):
    global_ids = first_slot + jnp.arange(slot_count, dtype=jnp.int32)
    match_int = (page_table[None, :, :] == global_ids[:, None, None]).astype(jnp.int32)
    request_ids = jnp.arange(page_table.shape[0], dtype=jnp.int32)
    page_ids = jnp.arange(page_table.shape[1], dtype=jnp.int32)
    owner_ids = jnp.sum(match_int * request_ids[None, :, None], axis=(1, 2))
    logical = jnp.sum(match_int * page_ids[None, None, :], axis=(1, 2))
    live_mask = jnp.sum(match_int, axis=(1, 2)) > 0
    return (owner_ids, logical, live_mask)


def page_partials(q_rows, key_pages, value_pages, owner_ids, logical, live_mask, kv_lengths):
    slot_count, heads_kv, page_len, head_dim = key_pages.shape
    group_width = q_rows.shape[1] // heads_kv
    slot_queries = jnp.take(q_rows, owner_ids, axis=0).reshape(
        slot_count, heads_kv, group_width, head_dim
    )
    scores = jnp.einsum(
        "skgd,sktd->skgt", slot_queries, key_pages, preferred_element_type=jnp.float32
    ) * head_dim ** (-0.5)
    positions = logical[:, None] * page_len + jnp.arange(page_len, dtype=jnp.int32)[None, :]
    valid_mask = live_mask[:, None] & (positions < jnp.take(kv_lengths, owner_ids)[:, None])
    valid_wide = valid_mask[:, None, None, :]
    masked = jnp.where(valid_wide, scores, NEG_BIG)
    page_max = jnp.max(masked, axis=3)
    weights = jnp.where(valid_wide, jnp.exp(masked - page_max[..., None]), 0.0)
    page_sum = jnp.sum(weights, axis=3)
    page_out = jnp.einsum(
        "skgt,sktd->skgd",
        weights.astype(jnp.bfloat16),
        value_pages,
        preferred_element_type=jnp.float32,
    )
    return (
        page_max.reshape(slot_count, -1),
        page_sum.reshape(slot_count, -1),
        page_out.reshape(slot_count, -1),
    )


def request_partials(page_max, page_sum, page_out, owner_ids, live_mask, requests, head_dim):
    slot_count, heads_local = page_max.shape
    owned = (owner_ids[:, None] == jnp.arange(requests, dtype=jnp.int32)[None, :]) & live_mask[
        :, None
    ]
    req_max = jnp.max(jnp.where(owned[:, :, None], page_max[:, None, :], NEG_BIG), axis=0)
    factor = jnp.where(
        live_mask[:, None], jnp.exp(page_max - jnp.take(req_max, owner_ids, axis=0)), 0.0
    )
    owned_float = owned.astype(jnp.float32)
    req_sum = jnp.einsum(
        "sr,sh->rh", owned_float, page_sum * factor, precision=lax.Precision.HIGHEST
    )
    scaled = (page_out.reshape(slot_count, heads_local, head_dim) * factor[..., None]).reshape(
        slot_count, -1
    )
    req_out = jnp.einsum("sr,sx->rx", owned_float, scaled, precision=lax.Precision.HIGHEST)
    return (req_max, req_sum, req_out.reshape(requests, heads_local, head_dim))


def plain_shards(queries, k_cache, value_cache, kv_lengths, page_table, request_batch_row):
    slot_count = k_cache.shape[0]
    requests = queries.shape[0]
    heads_local = queries.shape[1]
    head_dim = queries.shape[2]
    first_slot = lax.axis_index("seq") * slot_count
    owner_ids, logical, live_mask = slot_owners(page_table, first_slot, slot_count)
    q_rows = jnp.take(queries, request_batch_row, axis=0)
    page_max, page_sum, page_out = page_partials(
        q_rows, k_cache, value_cache, owner_ids, logical, live_mask, kv_lengths
    )
    owner_used, live_used = (owner_ids, live_mask)
    req_max, req_sum, req_out = request_partials(
        page_max, page_sum, page_out, owner_used, live_used, requests, head_dim
    )
    overall = lax.pmax(req_max, "seq")
    factor = jnp.exp(req_max - overall)
    flat_sum = (req_sum * factor).reshape(-1)
    flat_out = (req_out * factor[..., None]).reshape(requests * heads_local, head_dim)
    part_out, part_sum = (
        lax.psum_scatter(flat_out, "seq", scatter_dimension=0, tiled=True),
        lax.psum_scatter(flat_sum, "seq", scatter_dimension=0, tiled=True),
    )
    finished = (part_out / part_sum[:, None]).astype(jnp.bfloat16)
    result = lax.all_gather(finished, "seq", axis=0, tiled=True).reshape(
        requests, heads_local, head_dim
    )
    return jnp.zeros_like(queries).at[request_batch_row].set(result)


def attend_kernel(
    n,
    rows_smem,
    lens_smem,
    rows_ref,
    table_ref,
    q_hbm,
    k_hbm,
    v_hbm,
    out_ref,
    q_ref,
    k_buf,
    v_buf,
    part,
    x_send,
    x_recv,
    l_send,
    l_recv,
    piece,
    pieces,
    wide,
    q_sem,
    k_sem,
    v_sem,
    xs_sem,
    xr_sem,
    ls_sem,
    lr_sem,
    gs_sem,
    gr_sem,
    fs_sem,
    fr_sem,
):
    me = lax.axis_index("seq")
    slots, heads_kv, page_len, head_dim = k_hbm.shape
    requests, heads, _ = q_ref.shape
    width = heads // heads_kv
    mine = heads // n
    pages = table_ref.shape[1]
    total_slots = n * slots

    def remote(src, dst, send_sem, recv_sem, target):
        return pltpu.make_async_remote_copy(
            src_ref=src,
            dst_ref=dst,
            send_sem=send_sem,
            recv_sem=recv_sem,
            device_id={"seq": target},
            device_id_type=pl.DeviceIdType.MESH,
        )

    far_first = sorted(range(1, n), key=lambda o: abs(o - n // 2))
    q_copy = pltpu.make_async_copy(q_hbm, q_ref, q_sem)
    q_copy.start()
    barrier = pltpu.get_barrier_semaphore()
    for o in far_first:
        pl.semaphore_signal(
            barrier,
            inc=1,
            device_id={"seq": lax.rem(me + o, n)},
            device_id_type=pl.DeviceIdType.MESH,
        )

    k_copies = [pltpu.make_async_copy(k_hbm.at[s], k_buf.at[s], k_sem.at[s]) for s in range(slots)]
    v_copies = [pltpu.make_async_copy(v_hbm.at[s], v_buf.at[s], v_sem.at[s]) for s in range(slots)]
    for s in range(slots):
        k_copies[s].start()
        v_copies[s].start()

    table = table_ref[...]
    code = lax.broadcasted_iota(jnp.int32, table.shape, 0) * pages + lax.broadcasted_iota(
        jnp.int32, table.shape, 1
    )
    found = []
    for s in range(slots):
        found.append(jnp.max(jnp.where(table == me * slots + s, code, -1)))

    lane = lax.broadcasted_iota(jnp.int32, (1, total_slots), 1)
    token = lax.broadcasted_iota(jnp.int32, (1, page_len), 1)
    q_copy.wait()
    lse = jnp.zeros((heads, total_slots), jnp.float32)
    for s in range(slots):
        at = jnp.maximum(found[s], 0)
        request = at // pages
        page = at - request * pages
        left = jnp.where(found[s] >= 0, lens_smem[request] - page * page_len, 0)
        q_rows = q_ref[rows_smem[request]]
        k_copies[s].wait()
        scores = jnp.concatenate(
            [
                lax.dot_general(
                    q_rows[g * width : (g + 1) * width],
                    k_buf[s, g],
                    (((1,), (1,)), ((), ())),
                    preferred_element_type=jnp.float32,
                )
                for g in range(heads_kv)
            ],
            axis=0,
        ) * head_dim ** (-0.5)
        masked = jnp.where(token < left, scores, NEG_BIG)
        top = jnp.max(masked, axis=1, keepdims=True)
        weights = jnp.exp(masked - top)
        weight_sum = jnp.sum(weights, axis=1, keepdims=True)
        lse = jnp.where(lane == me * slots + s, top + jnp.log(weight_sum), lse)
        weights_bf = weights.astype(jnp.bfloat16)
        inverse = 1.0 / weight_sum
        v_copies[s].wait()
        for g in range(heads_kv):
            band = slice(g * width, (g + 1) * width)
            out = jnp.dot(weights_bf[band], v_buf[s, g], preferred_element_type=jnp.float32)
            part[band, s, :] = out * inverse[band]

    l_send[...] = lse.reshape(n, mine, total_slots)
    for j in range(n):
        x_send[j] = part[j * mine : (j + 1) * mine].astype(jnp.bfloat16)

    pl.semaphore_wait(barrier, n - 1)
    first = []
    for o in far_first:
        to = lax.rem(me + o, n)
        first.append(remote(l_send.at[to], l_recv.at[me], ls_sem.at[o], lr_sem.at[me], to))
        first.append(remote(x_send.at[to], x_recv.at[me], xs_sem.at[o], xr_sem.at[me], to))
    for copy in first:
        copy.start()

    x_recv[me] = x_send[me]
    l_recv[me] = l_send[me]
    owned = jnp.zeros((requests, total_slots), jnp.bool_)
    for p in range(pages):
        owned = owned | (table[:, p : p + 1] == lane)
    place = (
        lax.broadcasted_iota(jnp.int32, (requests, requests), 0) == rows_ref[...]
    ).astype(jnp.float32).astype(jnp.bfloat16)
    owned = (
        jnp.dot(
            place,
            owned.astype(jnp.float32).astype(jnp.bfloat16),
            preferred_element_type=jnp.float32,
        )
        > 0.5
    )

    for o in range(1, n):
        source = lax.rem(me + o, n)
        remote(l_send.at[0], l_recv.at[source], ls_sem.at[0], lr_sem.at[source], source).wait_recv()
    lse_all = l_recv[0]
    for j in range(1, n):
        lse_all = lse_all + l_recv[j]
    mixes = []
    for h in range(mine):
        level = jnp.where(owned, lse_all[h : h + 1], NEG_BIG)
        peak = jnp.max(level, axis=1, keepdims=True)
        mix = jnp.where(owned, jnp.exp(level - peak), 0.0)
        mix = mix * (1.0 / jnp.sum(mix, axis=1, keepdims=True))
        high = mix.astype(jnp.bfloat16)
        low = (mix - high.astype(jnp.float32)).astype(jnp.bfloat16)
        mixes.append((high, low))
    for o in range(1, n):
        source = lax.rem(me + o, n)
        remote(x_send.at[0], x_recv.at[source], xs_sem.at[0], xr_sem.at[source], source).wait_recv()
    for h in range(mine):
        rows = jnp.concatenate([x_recv[j, h].astype(jnp.float32) for j in range(n)], axis=0).astype(
            jnp.bfloat16
        )
        high, low = mixes[h]
        done = jnp.dot(high, rows, preferred_element_type=jnp.float32) + jnp.dot(
            low, rows, preferred_element_type=jnp.float32
        )
        piece[h] = done.astype(jnp.bfloat16)

    partner = me + 1 - 2 * lax.rem(me, 2)
    far_even = [o for o in far_first if o % 2 == 0]
    near_even = far_even[::-1]
    second = []
    for o in far_even:
        to = lax.rem(me + o, n)
        second.append(remote(piece, pieces.at[me], gs_sem.at[o], gr_sem.at[me], to))
    second.append(remote(piece, pieces.at[me], fs_sem.at[0], fr_sem.at[me], partner))
    for copy in second:
        copy.start()

    def spread(block, source):
        for h in range(mine):
            wide[:, source * mine + h, :] = block[h].astype(jnp.float32)

    spread(piece, me)
    passed = []
    for o in near_even:
        source = lax.rem(me + o, n)
        remote(piece, pieces.at[source], gs_sem.at[0], gr_sem.at[source], source).wait_recv()
        on = remote(pieces.at[source], pieces.at[source], fs_sem.at[o], fr_sem.at[source], partner)
        on.start()
        passed.append(on)
        spread(pieces.at[source], source)
    for o in [0] + near_even:
        source = lax.rem(partner + o, n)
        remote(piece, pieces.at[source], fs_sem.at[0], fr_sem.at[source], partner).wait_recv()
        spread(pieces.at[source], source)
    out_ref[...] = wide[...].astype(out_ref.dtype)
    for copy in first + second + passed:
        copy.wait_send()


def seq_shards(n, queries, k_cache, value_cache, kv_lengths, page_table, request_batch_row):
    slots, heads_kv, page_len, head_dim = k_cache.shape
    requests, heads, _ = queries.shape
    if heads % n or n % 2:
        return plain_shards(
            queries, k_cache, value_cache, kv_lengths, page_table, request_batch_row
        )
    mine = heads // n
    smem = pl.BlockSpec(memory_space=pltpu.SMEM)
    vmem = pl.BlockSpec(memory_space=pltpu.VMEM)
    anywhere = pl.BlockSpec(memory_space=pl.ANY)
    sems = pltpu.SemaphoreType.DMA
    out = pl.pallas_call(
        functools.partial(attend_kernel, n),
        out_shape=pltpu.VMEM(queries.shape, queries.dtype),
        in_specs=[smem, smem, vmem, vmem, anywhere, anywhere, anywhere],
        out_specs=vmem,
        scratch_shapes=[
            pltpu.VMEM(queries.shape, queries.dtype),
            pltpu.VMEM(k_cache.shape, k_cache.dtype),
            pltpu.VMEM(value_cache.shape, value_cache.dtype),
            pltpu.VMEM((heads, slots, head_dim), jnp.float32),
            pltpu.VMEM((n, mine, slots, head_dim), jnp.bfloat16),
            pltpu.VMEM((n, mine, slots, head_dim), jnp.bfloat16),
            pltpu.VMEM((n, mine, n * slots), jnp.float32),
            pltpu.VMEM((n, mine, n * slots), jnp.float32),
            pltpu.VMEM((mine, requests, head_dim), jnp.bfloat16),
            pltpu.VMEM((n, mine, requests, head_dim), jnp.bfloat16),
            pltpu.VMEM(queries.shape, jnp.float32),
            sems,
            sems((slots,)),
            sems((slots,)),
            sems((n,)),
            sems((n,)),
            sems((n,)),
            sems((n,)),
            sems((n,)),
            sems((n,)),
            sems((n,)),
            sems((n,)),
        ],
        compiler_params=pltpu.CompilerParams(collective_id=0, has_side_effects=True),
    )(
        request_batch_row,
        kv_lengths,
        request_batch_row.reshape(1, requests),
        page_table,
        queries,
        k_cache,
        value_cache,
    )
    return out


def solution(mesh):
    shards = functools.partial(seq_shards, mesh.shape["seq"])
    return jax.shard_map(
        shards,
        mesh=mesh,
        in_specs=(
            P("group", "tensor", None),
            P(("group", "seq"), "tensor", None, None),
            P(("group", "seq"), "tensor", None, None),
            P("group"),
            P("group", None),
            P("group"),
        ),
        out_specs=P("group", "tensor", None),
        check_vma=False,
    )
```

```python
import functools

import jax
import jax.numpy as jnp
from jax import lax
from jax.experimental import pallas as pl
from jax.experimental.pallas import tpu as pltpu
from jax.sharding import PartitionSpec as P

NEG_BIG = -1e30


def slot_owners(page_table, first_slot, slot_count):
    global_ids = first_slot + jnp.arange(slot_count, dtype=jnp.int32)
    match_int = (page_table[None, :, :] == global_ids[:, None, None]).astype(jnp.int32)
    request_ids = jnp.arange(page_table.shape[0], dtype=jnp.int32)
    page_ids = jnp.arange(page_table.shape[1], dtype=jnp.int32)
    owner_ids = jnp.sum(match_int * request_ids[None, :, None], axis=(1, 2))
    logical = jnp.sum(match_int * page_ids[None, None, :], axis=(1, 2))
    live_mask = jnp.sum(match_int, axis=(1, 2)) > 0
    return (owner_ids, logical, live_mask)


def page_partials(q_rows, key_pages, value_pages, owner_ids, logical, live_mask, kv_lengths):
    slot_count, heads_kv, page_len, head_dim = key_pages.shape
    group_width = q_rows.shape[1] // heads_kv
    slot_queries = jnp.take(q_rows, owner_ids, axis=0).reshape(
        slot_count, heads_kv, group_width, head_dim
    )
    scores = jnp.einsum(
        "skgd,sktd->skgt", slot_queries, key_pages, preferred_element_type=jnp.float32
    ) * head_dim ** (-0.5)
    positions = logical[:, None] * page_len + jnp.arange(page_len, dtype=jnp.int32)[None, :]
    valid_mask = live_mask[:, None] & (positions < jnp.take(kv_lengths, owner_ids)[:, None])
    valid_wide = valid_mask[:, None, None, :]
    masked = jnp.where(valid_wide, scores, NEG_BIG)
    page_max = jnp.max(masked, axis=3)
    weights = jnp.where(valid_wide, jnp.exp(masked - page_max[..., None]), 0.0)
    page_sum = jnp.sum(weights, axis=3)
    page_out = jnp.einsum(
        "skgt,sktd->skgd",
        weights.astype(jnp.bfloat16),
        value_pages,
        preferred_element_type=jnp.float32,
    )
    return (
        page_max.reshape(slot_count, -1),
        page_sum.reshape(slot_count, -1),
        page_out.reshape(slot_count, -1),
    )


def request_partials(page_max, page_sum, page_out, owner_ids, live_mask, requests, head_dim):
    slot_count, heads_local = page_max.shape
    owned = (owner_ids[:, None] == jnp.arange(requests, dtype=jnp.int32)[None, :]) & live_mask[
        :, None
    ]
    req_max = jnp.max(jnp.where(owned[:, :, None], page_max[:, None, :], NEG_BIG), axis=0)
    factor = jnp.where(
        live_mask[:, None], jnp.exp(page_max - jnp.take(req_max, owner_ids, axis=0)), 0.0
    )
    owned_float = owned.astype(jnp.float32)
    req_sum = jnp.einsum(
        "sr,sh->rh", owned_float, page_sum * factor, precision=lax.Precision.HIGHEST
    )
    scaled = (page_out.reshape(slot_count, heads_local, head_dim) * factor[..., None]).reshape(
        slot_count, -1
    )
    req_out = jnp.einsum("sr,sx->rx", owned_float, scaled, precision=lax.Precision.HIGHEST)
    return (req_max, req_sum, req_out.reshape(requests, heads_local, head_dim))


def plain_shards(queries, k_cache, value_cache, kv_lengths, page_table, request_batch_row):
    slot_count = k_cache.shape[0]
    requests = queries.shape[0]
    heads_local = queries.shape[1]
    head_dim = queries.shape[2]
    first_slot = lax.axis_index("seq") * slot_count
    owner_ids, logical, live_mask = slot_owners(page_table, first_slot, slot_count)
    q_rows = jnp.take(queries, request_batch_row, axis=0)
    page_max, page_sum, page_out = page_partials(
        q_rows, k_cache, value_cache, owner_ids, logical, live_mask, kv_lengths
    )
    owner_used, live_used = (owner_ids, live_mask)
    req_max, req_sum, req_out = request_partials(
        page_max, page_sum, page_out, owner_used, live_used, requests, head_dim
    )
    overall = lax.pmax(req_max, "seq")
    factor = jnp.exp(req_max - overall)
    flat_sum = (req_sum * factor).reshape(-1)
    flat_out = (req_out * factor[..., None]).reshape(requests * heads_local, head_dim)
    part_out, part_sum = (
        lax.psum_scatter(flat_out, "seq", scatter_dimension=0, tiled=True),
        lax.psum_scatter(flat_sum, "seq", scatter_dimension=0, tiled=True),
    )
    finished = (part_out / part_sum[:, None]).astype(jnp.bfloat16)
    result = lax.all_gather(finished, "seq", axis=0, tiled=True).reshape(
        requests, heads_local, head_dim
    )
    return jnp.zeros_like(queries).at[request_batch_row].set(result)


BATCHES = 1


def attend_kernel(
    n,
    rows_smem,
    lens_smem,
    rows_ref,
    table_ref,
    q_hbm,
    k_hbm,
    v_hbm,
    out_ref,
    q_ref,
    k_buf,
    v_buf,
    part,
    x_send,
    x_recv,
    l_send,
    l_recv,
    piece,
    pieces,
    wide,
    q_sem,
    k_sem,
    v_sem,
    xs_sem,
    xr_sem,
    ls_sem,
    lr_sem,
    gs_sem,
    gr_sem,
    fs_sem,
    fr_sem,
):
    me = lax.axis_index("seq")
    slots, heads_kv, page_len, head_dim = k_hbm.shape
    requests, heads, _ = q_ref.shape
    width = heads // heads_kv
    mine = heads // n
    pages = table_ref.shape[1]
    total_slots = n * slots

    def remote(src, dst, send_sem, recv_sem, target):
        return pltpu.make_async_remote_copy(
            src_ref=src,
            dst_ref=dst,
            send_sem=send_sem,
            recv_sem=recv_sem,
            device_id={"seq": target},
            device_id_type=pl.DeviceIdType.MESH,
        )

    far_first = sorted(range(1, n), key=lambda o: abs(o - n // 2))
    q_copy = pltpu.make_async_copy(q_hbm, q_ref, q_sem)
    q_copy.start()
    barrier = pltpu.get_barrier_semaphore()
    for o in far_first:
        pl.semaphore_signal(
            barrier,
            inc=1,
            device_id={"seq": lax.rem(me + o, n)},
            device_id_type=pl.DeviceIdType.MESH,
        )

    batch = slots // BATCHES if slots % BATCHES == 0 else slots
    batches = [range(at, at + batch) for at in range(0, slots, batch)]

    def fetch(source, buffer, sem):
        copies = []
        for i in range(len(batches)):
            some = pl.ds(i * batch, batch)
            copies.append(pltpu.make_async_copy(source.at[some], buffer.at[some], sem.at[i]))
        return copies

    k_copies = fetch(k_hbm, k_buf, k_sem)
    v_copies = fetch(v_hbm, v_buf, v_sem)
    for copy in k_copies + v_copies:
        copy.start()

    table = table_ref[...]
    code = lax.broadcasted_iota(jnp.int32, table.shape, 0) * pages + lax.broadcasted_iota(
        jnp.int32, table.shape, 1
    )
    found = []
    for s in range(slots):
        found.append(jnp.max(jnp.where(table == me * slots + s, code, -1)))

    lane = lax.broadcasted_iota(jnp.int32, (1, total_slots), 1)
    token = lax.broadcasted_iota(jnp.int32, (1, page_len), 1)
    q_copy.wait()
    lse = jnp.zeros((heads, total_slots), jnp.float32)
    kept = []
    for i, some in enumerate(batches):
        k_copies[i].wait()
        for s in some:
            at = jnp.maximum(found[s], 0)
            request = at // pages
            page = at - request * pages
            left = jnp.where(found[s] >= 0, lens_smem[request] - page * page_len, 0)
            row = rows_smem[request]
            scores = jnp.concatenate(
                [
                    lax.dot_general(
                        q_ref[row, g * width : (g + 1) * width, :],
                        k_buf[s, g],
                        (((1,), (1,)), ((), ())),
                        preferred_element_type=jnp.float32,
                    )
                    for g in range(heads_kv)
                ],
                axis=0,
            ) * head_dim ** (-0.5)
            masked = jnp.where(token < left, scores, NEG_BIG)
            top = jnp.max(masked, axis=1, keepdims=True)
            weights = jnp.exp(masked - top)
            weight_sum = jnp.sum(weights, axis=1, keepdims=True)
            lse = jnp.where(lane == me * slots + s, top + jnp.log(weight_sum), lse)
            kept.append((weights.astype(jnp.bfloat16), 1.0 / weight_sum))
    for i, some in enumerate(batches):
        v_copies[i].wait()
        for s in some:
            weights_bf, inverse = kept[s]
            for g in range(heads_kv):
                band = slice(g * width, (g + 1) * width)
                out = jnp.dot(weights_bf[band], v_buf[s, g], preferred_element_type=jnp.float32)
                part[band, s, :] = out * inverse[band]

    l_send[...] = lse.reshape(n, mine, total_slots)
    for j in range(n):
        x_send[j] = part[j * mine : (j + 1) * mine].astype(jnp.bfloat16)

    pl.semaphore_wait(barrier, n - 1)
    first = []
    for o in far_first:
        to = lax.rem(me + o, n)
        first.append(remote(l_send.at[to], l_recv.at[me], ls_sem.at[o], lr_sem.at[me], to))
        first.append(remote(x_send.at[to], x_recv.at[me], xs_sem.at[o], xr_sem.at[me], to))
    for copy in first:
        copy.start()

    x_recv[me] = x_send[me]
    l_recv[me] = l_send[me]
    owned = jnp.zeros((requests, total_slots), jnp.bool_)
    for p in range(pages):
        owned = owned | (table[:, p : p + 1] == lane)
    place = (
        lax.broadcasted_iota(jnp.int32, (requests, requests), 0) == rows_ref[...]
    ).astype(jnp.float32).astype(jnp.bfloat16)
    owned = (
        jnp.dot(
            place,
            owned.astype(jnp.float32).astype(jnp.bfloat16),
            preferred_element_type=jnp.float32,
        )
        > 0.5
    )

    for o in range(1, n):
        source = lax.rem(me + o, n)
        remote(l_send.at[0], l_recv.at[source], ls_sem.at[0], lr_sem.at[source], source).wait_recv()
    lse_all = l_recv[0]
    for j in range(1, n):
        lse_all = lse_all + l_recv[j]
    mixes = []
    for h in range(mine):
        level = jnp.where(owned, lse_all[h : h + 1], NEG_BIG)
        peak = jnp.max(level, axis=1, keepdims=True)
        mix = jnp.where(owned, jnp.exp(level - peak), 0.0)
        mix = mix * (1.0 / jnp.sum(mix, axis=1, keepdims=True))
        high = mix.astype(jnp.bfloat16)
        low = (mix - high.astype(jnp.float32)).astype(jnp.bfloat16)
        mixes.append((high, low))
    for o in range(1, n):
        source = lax.rem(me + o, n)
        remote(x_send.at[0], x_recv.at[source], xs_sem.at[0], xr_sem.at[source], source).wait_recv()
    for h in range(mine):
        rows = jnp.concatenate([x_recv[j, h].astype(jnp.float32) for j in range(n)], axis=0).astype(
            jnp.bfloat16
        )
        high, low = mixes[h]
        done = jnp.dot(high, rows, preferred_element_type=jnp.float32) + jnp.dot(
            low, rows, preferred_element_type=jnp.float32
        )
        piece[h] = done.astype(jnp.bfloat16)

    partner = me + 1 - 2 * lax.rem(me, 2)
    far_even = [o for o in far_first if o % 2 == 0]
    near_even = far_even[::-1]
    second = []
    for o in far_even:
        to = lax.rem(me + o, n)
        second.append(remote(piece, pieces.at[me], gs_sem.at[o], gr_sem.at[me], to))
    second.append(remote(piece, pieces.at[me], fs_sem.at[0], fr_sem.at[me], partner))
    for copy in second:
        copy.start()

    def spread(block, source):
        for h in range(mine):
            wide[:, source * mine + h, :] = block[h].astype(jnp.float32)

    spread(piece, me)
    passed = []
    for o in near_even:
        source = lax.rem(me + o, n)
        remote(piece, pieces.at[source], gs_sem.at[0], gr_sem.at[source], source).wait_recv()
        on = remote(pieces.at[source], pieces.at[source], fs_sem.at[o], fr_sem.at[source], partner)
        on.start()
        passed.append(on)
        spread(pieces.at[source], source)
    for o in [0] + near_even:
        source = lax.rem(partner + o, n)
        remote(piece, pieces.at[source], fs_sem.at[0], fr_sem.at[source], partner).wait_recv()
        spread(pieces.at[source], source)
    out_ref[...] = wide[...].astype(out_ref.dtype)
    for copy in first + second + passed:
        copy.wait_send()


def seq_shards(n, queries, k_cache, value_cache, kv_lengths, page_table, request_batch_row):
    slots, heads_kv, page_len, head_dim = k_cache.shape
    requests, heads, _ = queries.shape
    if heads % n or n % 2:
        return plain_shards(
            queries, k_cache, value_cache, kv_lengths, page_table, request_batch_row
        )
    mine = heads // n
    smem = pl.BlockSpec(memory_space=pltpu.SMEM)
    vmem = pl.BlockSpec(memory_space=pltpu.VMEM)
    anywhere = pl.BlockSpec(memory_space=pl.ANY)
    sems = pltpu.SemaphoreType.DMA
    out = pl.pallas_call(
        functools.partial(attend_kernel, n),
        out_shape=pltpu.VMEM(queries.shape, queries.dtype),
        in_specs=[smem, smem, vmem, vmem, anywhere, anywhere, anywhere],
        out_specs=vmem,
        scratch_shapes=[
            pltpu.VMEM(queries.shape, queries.dtype),
            pltpu.VMEM(k_cache.shape, k_cache.dtype),
            pltpu.VMEM(value_cache.shape, value_cache.dtype),
            pltpu.VMEM((heads, slots, head_dim), jnp.float32),
            pltpu.VMEM((n, mine, slots, head_dim), jnp.bfloat16),
            pltpu.VMEM((n, mine, slots, head_dim), jnp.bfloat16),
            pltpu.VMEM((n, mine, n * slots), jnp.float32),
            pltpu.VMEM((n, mine, n * slots), jnp.float32),
            pltpu.VMEM((mine, requests, head_dim), jnp.bfloat16),
            pltpu.VMEM((n, mine, requests, head_dim), jnp.bfloat16),
            pltpu.VMEM(queries.shape, jnp.float32),
            sems,
            sems((slots,)),
            sems((slots,)),
            sems((n,)),
            sems((n,)),
            sems((n,)),
            sems((n,)),
            sems((n,)),
            sems((n,)),
            sems((n,)),
            sems((n,)),
        ],
        compiler_params=pltpu.CompilerParams(collective_id=0, has_side_effects=True),
    )(
        request_batch_row,
        kv_lengths,
        request_batch_row.reshape(1, requests),
        page_table,
        queries,
        k_cache,
        value_cache,
    )
    return out


def solution(mesh):
    shards = functools.partial(seq_shards, mesh.shape["seq"])
    return jax.shard_map(
        shards,
        mesh=mesh,
        in_specs=(
            P("group", "tensor", None),
            P(("group", "seq"), "tensor", None, None),
            P(("group", "seq"), "tensor", None, None),
            P("group"),
            P("group", None),
            P("group"),
        ),
        out_specs=P("group", "tensor", None),
        check_vma=False,
    )
```

```python
import functools

import jax
import jax.numpy as jnp
from jax import lax
from jax.experimental import pallas as pl
from jax.experimental.pallas import tpu as pltpu
from jax.sharding import PartitionSpec as P

NEG_BIG = -1e30


def slot_owners(page_table, first_slot, slot_count):
    global_ids = first_slot + jnp.arange(slot_count, dtype=jnp.int32)
    match_int = (page_table[None, :, :] == global_ids[:, None, None]).astype(jnp.int32)
    request_ids = jnp.arange(page_table.shape[0], dtype=jnp.int32)
    page_ids = jnp.arange(page_table.shape[1], dtype=jnp.int32)
    owner_ids = jnp.sum(match_int * request_ids[None, :, None], axis=(1, 2))
    logical = jnp.sum(match_int * page_ids[None, None, :], axis=(1, 2))
    live_mask = jnp.sum(match_int, axis=(1, 2)) > 0
    return (owner_ids, logical, live_mask)


def page_partials(q_rows, key_pages, value_pages, owner_ids, logical, live_mask, kv_lengths):
    slot_count, heads_kv, page_len, head_dim = key_pages.shape
    group_width = q_rows.shape[1] // heads_kv
    slot_queries = jnp.take(q_rows, owner_ids, axis=0).reshape(
        slot_count, heads_kv, group_width, head_dim
    )
    scores = jnp.einsum(
        "skgd,sktd->skgt", slot_queries, key_pages, preferred_element_type=jnp.float32
    ) * head_dim ** (-0.5)
    positions = logical[:, None] * page_len + jnp.arange(page_len, dtype=jnp.int32)[None, :]
    valid_mask = live_mask[:, None] & (positions < jnp.take(kv_lengths, owner_ids)[:, None])
    valid_wide = valid_mask[:, None, None, :]
    masked = jnp.where(valid_wide, scores, NEG_BIG)
    page_max = jnp.max(masked, axis=3)
    weights = jnp.where(valid_wide, jnp.exp(masked - page_max[..., None]), 0.0)
    page_sum = jnp.sum(weights, axis=3)
    page_out = jnp.einsum(
        "skgt,sktd->skgd",
        weights.astype(jnp.bfloat16),
        value_pages,
        preferred_element_type=jnp.float32,
    )
    return (
        page_max.reshape(slot_count, -1),
        page_sum.reshape(slot_count, -1),
        page_out.reshape(slot_count, -1),
    )


def request_partials(page_max, page_sum, page_out, owner_ids, live_mask, requests, head_dim):
    slot_count, heads_local = page_max.shape
    owned = (owner_ids[:, None] == jnp.arange(requests, dtype=jnp.int32)[None, :]) & live_mask[
        :, None
    ]
    req_max = jnp.max(jnp.where(owned[:, :, None], page_max[:, None, :], NEG_BIG), axis=0)
    factor = jnp.where(
        live_mask[:, None], jnp.exp(page_max - jnp.take(req_max, owner_ids, axis=0)), 0.0
    )
    owned_float = owned.astype(jnp.float32)
    req_sum = jnp.einsum(
        "sr,sh->rh", owned_float, page_sum * factor, precision=lax.Precision.HIGHEST
    )
    scaled = (page_out.reshape(slot_count, heads_local, head_dim) * factor[..., None]).reshape(
        slot_count, -1
    )
    req_out = jnp.einsum("sr,sx->rx", owned_float, scaled, precision=lax.Precision.HIGHEST)
    return (req_max, req_sum, req_out.reshape(requests, heads_local, head_dim))


def plain_shards(queries, k_cache, value_cache, kv_lengths, page_table, request_batch_row):
    slot_count = k_cache.shape[0]
    requests = queries.shape[0]
    heads_local = queries.shape[1]
    head_dim = queries.shape[2]
    first_slot = lax.axis_index("seq") * slot_count
    owner_ids, logical, live_mask = slot_owners(page_table, first_slot, slot_count)
    q_rows = jnp.take(queries, request_batch_row, axis=0)
    page_max, page_sum, page_out = page_partials(
        q_rows, k_cache, value_cache, owner_ids, logical, live_mask, kv_lengths
    )
    owner_used, live_used = (owner_ids, live_mask)
    req_max, req_sum, req_out = request_partials(
        page_max, page_sum, page_out, owner_used, live_used, requests, head_dim
    )
    overall = lax.pmax(req_max, "seq")
    factor = jnp.exp(req_max - overall)
    flat_sum = (req_sum * factor).reshape(-1)
    flat_out = (req_out * factor[..., None]).reshape(requests * heads_local, head_dim)
    part_out, part_sum = (
        lax.psum_scatter(flat_out, "seq", scatter_dimension=0, tiled=True),
        lax.psum_scatter(flat_sum, "seq", scatter_dimension=0, tiled=True),
    )
    finished = (part_out / part_sum[:, None]).astype(jnp.bfloat16)
    result = lax.all_gather(finished, "seq", axis=0, tiled=True).reshape(
        requests, heads_local, head_dim
    )
    return jnp.zeros_like(queries).at[request_batch_row].set(result)


BATCHES = 1


def attend_kernel(
    n,
    rows_hbm,
    lens_hbm,
    line_hbm,
    table_hbm,
    q_hbm,
    k_hbm,
    v_hbm,
    out_ref,
    rows_smem,
    lens_smem,
    rows_ref,
    table_ref,
    q_ref,
    k_buf,
    v_buf,
    part,
    x_send,
    x_recv,
    l_send,
    l_recv,
    piece,
    pieces,
    wide,
    small_sem,
    q_sem,
    k_sem,
    v_sem,
    xs_sem,
    xr_sem,
    ls_sem,
    lr_sem,
    gs_sem,
    gr_sem,
    fs_sem,
    fr_sem,
):
    me = lax.axis_index("seq")
    slots, heads_kv, page_len, head_dim = k_hbm.shape
    requests, heads, _ = q_ref.shape
    width = heads // heads_kv
    mine = heads // n
    pages = table_ref.shape[1]
    total_slots = n * slots

    def remote(src, dst, send_sem, recv_sem, target):
        return pltpu.make_async_remote_copy(
            src_ref=src,
            dst_ref=dst,
            send_sem=send_sem,
            recv_sem=recv_sem,
            device_id={"seq": target},
            device_id_type=pl.DeviceIdType.MESH,
        )

    small = [
        pltpu.make_async_copy(table_hbm, table_ref, small_sem.at[0]),
        pltpu.make_async_copy(rows_hbm, rows_smem, small_sem.at[1]),
        pltpu.make_async_copy(lens_hbm, lens_smem, small_sem.at[2]),
        pltpu.make_async_copy(line_hbm, rows_ref, small_sem.at[3]),
    ]
    far_first = sorted(range(1, n), key=lambda o: abs(o - n // 2))
    q_copy = pltpu.make_async_copy(q_hbm, q_ref, q_sem)
    barrier = pltpu.get_barrier_semaphore()
    for o in far_first:
        pl.semaphore_signal(
            barrier,
            inc=1,
            device_id={"seq": lax.rem(me + o, n)},
            device_id_type=pl.DeviceIdType.MESH,
        )

    batch = slots // BATCHES if slots % BATCHES == 0 else slots
    batches = [range(at, at + batch) for at in range(0, slots, batch)]

    def fetch(source, buffer, sem):
        copies = []
        for i in range(len(batches)):
            some = pl.ds(i * batch, batch)
            copies.append(pltpu.make_async_copy(source.at[some], buffer.at[some], sem.at[i]))
        return copies

    k_copies = fetch(k_hbm, k_buf, k_sem)
    v_copies = fetch(v_hbm, v_buf, v_sem)
    for copy in small + [q_copy] + k_copies + v_copies:
        copy.start()
    for copy in small:
        copy.wait()

    table = table_ref[...]
    code = lax.broadcasted_iota(jnp.int32, table.shape, 0) * pages + lax.broadcasted_iota(
        jnp.int32, table.shape, 1
    )
    found = []
    for s in range(slots):
        found.append(jnp.max(jnp.where(table == me * slots + s, code, -1)))

    lane = lax.broadcasted_iota(jnp.int32, (1, total_slots), 1)
    token = lax.broadcasted_iota(jnp.int32, (1, page_len), 1)
    q_copy.wait()
    lse = jnp.zeros((heads, total_slots), jnp.float32)
    kept = []
    for i, some in enumerate(batches):
        k_copies[i].wait()
        for s in some:
            at = jnp.maximum(found[s], 0)
            request = at // pages
            page = at - request * pages
            left = jnp.where(found[s] >= 0, lens_smem[request] - page * page_len, 0)
            row = rows_smem[request]
            scores = jnp.concatenate(
                [
                    lax.dot_general(
                        q_ref[row, g * width : (g + 1) * width, :],
                        k_buf[s, g],
                        (((1,), (1,)), ((), ())),
                        preferred_element_type=jnp.float32,
                    )
                    for g in range(heads_kv)
                ],
                axis=0,
            ) * head_dim ** (-0.5)
            masked = jnp.where(token < left, scores, NEG_BIG)
            top = jnp.max(masked, axis=1, keepdims=True)
            weights = jnp.exp(masked - top)
            weight_sum = jnp.sum(weights, axis=1, keepdims=True)
            lse = jnp.where(lane == me * slots + s, top + jnp.log(weight_sum), lse)
            kept.append((weights.astype(jnp.bfloat16), 1.0 / weight_sum))
    for i, some in enumerate(batches):
        v_copies[i].wait()
        for s in some:
            weights_bf, inverse = kept[s]
            for g in range(heads_kv):
                band = slice(g * width, (g + 1) * width)
                out = jnp.dot(weights_bf[band], v_buf[s, g], preferred_element_type=jnp.float32)
                part[band, s, :] = out * inverse[band]

    l_send[...] = lse.reshape(n, mine, total_slots)
    for j in range(n):
        x_send[j] = part[j * mine : (j + 1) * mine].astype(jnp.bfloat16)

    pl.semaphore_wait(barrier, n - 1)
    first = []
    for o in far_first:
        to = lax.rem(me + o, n)
        first.append(remote(l_send.at[to], l_recv.at[me], ls_sem.at[o], lr_sem.at[me], to))
        first.append(remote(x_send.at[to], x_recv.at[me], xs_sem.at[o], xr_sem.at[me], to))
    for copy in first:
        copy.start()

    x_recv[me] = x_send[me]
    l_recv[me] = l_send[me]
    owned = jnp.zeros((requests, total_slots), jnp.bool_)
    for p in range(pages):
        owned = owned | (table[:, p : p + 1] == lane)
    place = (
        lax.broadcasted_iota(jnp.int32, (requests, requests), 0) == rows_ref[...]
    ).astype(jnp.float32).astype(jnp.bfloat16)
    owned = (
        jnp.dot(
            place,
            owned.astype(jnp.float32).astype(jnp.bfloat16),
            preferred_element_type=jnp.float32,
        )
        > 0.5
    )

    for o in range(1, n):
        source = lax.rem(me + o, n)
        remote(l_send.at[0], l_recv.at[source], ls_sem.at[0], lr_sem.at[source], source).wait_recv()
    lse_all = l_recv[0]
    for j in range(1, n):
        lse_all = lse_all + l_recv[j]
    mixes = []
    for h in range(mine):
        level = jnp.where(owned, lse_all[h : h + 1], NEG_BIG)
        peak = jnp.max(level, axis=1, keepdims=True)
        mix = jnp.where(owned, jnp.exp(level - peak), 0.0)
        mix = mix * (1.0 / jnp.sum(mix, axis=1, keepdims=True))
        high = mix.astype(jnp.bfloat16)
        low = (mix - high.astype(jnp.float32)).astype(jnp.bfloat16)
        mixes.append((high, low))
    for o in range(1, n):
        source = lax.rem(me + o, n)
        remote(x_send.at[0], x_recv.at[source], xs_sem.at[0], xr_sem.at[source], source).wait_recv()
    for h in range(mine):
        rows = jnp.concatenate([x_recv[j, h].astype(jnp.float32) for j in range(n)], axis=0).astype(
            jnp.bfloat16
        )
        high, low = mixes[h]
        done = jnp.dot(high, rows, preferred_element_type=jnp.float32) + jnp.dot(
            low, rows, preferred_element_type=jnp.float32
        )
        piece[h] = done.astype(jnp.bfloat16)

    partner = me + 1 - 2 * lax.rem(me, 2)
    far_even = [o for o in far_first if o % 2 == 0]
    near_even = far_even[::-1]
    second = []
    for o in far_even:
        to = lax.rem(me + o, n)
        second.append(remote(piece, pieces.at[me], gs_sem.at[o], gr_sem.at[me], to))
    second.append(remote(piece, pieces.at[me], fs_sem.at[0], fr_sem.at[me], partner))
    for copy in second:
        copy.start()

    def spread(block, source):
        for h in range(mine):
            wide[:, source * mine + h, :] = block[h].astype(jnp.float32)

    spread(piece, me)
    passed = []
    for o in near_even:
        source = lax.rem(me + o, n)
        remote(piece, pieces.at[source], gs_sem.at[0], gr_sem.at[source], source).wait_recv()
        on = remote(pieces.at[source], pieces.at[source], fs_sem.at[o], fr_sem.at[source], partner)
        on.start()
        passed.append(on)
        spread(pieces.at[source], source)
    for o in [0] + near_even:
        source = lax.rem(partner + o, n)
        remote(piece, pieces.at[source], fs_sem.at[0], fr_sem.at[source], partner).wait_recv()
        spread(pieces.at[source], source)
    out_ref[...] = wide[...].astype(out_ref.dtype)
    for copy in first + second + passed:
        copy.wait_send()


def seq_shards(n, queries, k_cache, value_cache, kv_lengths, page_table, request_batch_row):
    slots, heads_kv, page_len, head_dim = k_cache.shape
    requests, heads, _ = queries.shape
    if heads % n or n % 2:
        return plain_shards(
            queries, k_cache, value_cache, kv_lengths, page_table, request_batch_row
        )
    mine = heads // n
    vmem = pl.BlockSpec(memory_space=pltpu.VMEM)
    anywhere = pl.BlockSpec(memory_space=pl.ANY)
    sems = pltpu.SemaphoreType.DMA
    out = pl.pallas_call(
        functools.partial(attend_kernel, n),
        out_shape=pltpu.VMEM(queries.shape, queries.dtype),
        in_specs=[anywhere] * 7,
        out_specs=vmem,
        scratch_shapes=[
            pltpu.SMEM(request_batch_row.shape, jnp.int32),
            pltpu.SMEM(kv_lengths.shape, jnp.int32),
            pltpu.VMEM((1, requests), jnp.int32),
            pltpu.VMEM(page_table.shape, jnp.int32),
            pltpu.VMEM(queries.shape, queries.dtype),
            pltpu.VMEM(k_cache.shape, k_cache.dtype),
            pltpu.VMEM(value_cache.shape, value_cache.dtype),
            pltpu.VMEM((heads, slots, head_dim), jnp.float32),
            pltpu.VMEM((n, mine, slots, head_dim), jnp.bfloat16),
            pltpu.VMEM((n, mine, slots, head_dim), jnp.bfloat16),
            pltpu.VMEM((n, mine, n * slots), jnp.float32),
            pltpu.VMEM((n, mine, n * slots), jnp.float32),
            pltpu.VMEM((mine, requests, head_dim), jnp.bfloat16),
            pltpu.VMEM((n, mine, requests, head_dim), jnp.bfloat16),
            pltpu.VMEM(queries.shape, jnp.float32),
            sems((4,)),
            sems,
            sems((slots,)),
            sems((slots,)),
            sems((n,)),
            sems((n,)),
            sems((n,)),
            sems((n,)),
            sems((n,)),
            sems((n,)),
            sems((n,)),
            sems((n,)),
        ],
        compiler_params=pltpu.CompilerParams(collective_id=0, has_side_effects=True),
    )(
        request_batch_row,
        kv_lengths,
        request_batch_row.reshape(1, requests),
        page_table,
        queries,
        k_cache,
        value_cache,
    )
    return out


def solution(mesh):
    shards = functools.partial(seq_shards, mesh.shape["seq"])
    return jax.shard_map(
        shards,
        mesh=mesh,
        in_specs=(
            P("group", "tensor", None),
            P(("group", "seq"), "tensor", None, None),
            P(("group", "seq"), "tensor", None, None),
            P("group"),
            P("group", None),
            P("group"),
        ),
        out_specs=P("group", "tensor", None),
        check_vma=False,
    )
```
